32 devices in a mesh: tensor: 4 (over y, core), context: 8 (over z, x).
Axes of the slice: x: 2, y: 2, z: 4, core: 2. Of those that a mesh axis runs over, the one named last changes fastest.
Arguments:
- query_rows: bfloat16 [2048, 8192], P('context', 'tensor'), may hold values from -160 to 160, as said below
- key_rows: bfloat16 [2048, 1024], P('context'), may hold values from -5 to 5, as said below
- value_rows: bfloat16 [2048, 1024], P('context'), may hold values from -6 to 6
- doc_ids: int32 [2048], P('context'), may hold values from 0 to 3, never falling along the last dimension, each value on 1 to 1024 neighbouring positions
- out_weight: bfloat16 [8192, 8192], P('tensor'), may hold values from -0.09375 to 0.09375
Outputs:
- mixed: bfloat16 [2048, 8192], P('context', 'tensor')
The draws below stay inside these ranges and needn't reach their ends.
Inputs may be any that keep to these rules, and one draw needn't show every extreme that they name: `query_rows`: within the range given by the table of arrays. `key_rows`: within the range given by the table of arrays. `doc_ids`: document numbers never fall along the sequence; every document has 1 to 1024 tokens and one has exactly 1024.
All inputs are finite; a program needn't handle non-finite values.
Results may differ from the reference program's by a relative error of at most 0.015.
Values may be sent and summed in bfloat16 or wider, within the bound.
A program may use at most 128 MiB of HBM per device.

```python
import math
import jax
import jax.numpy as jnp
import numpy as np
from jax import lax

D = 8192
H = 64
KVH = 8
HD = 128
TOK_DEV = 256
DOC_MOST = 1024
TOKENS = 2048
DOCS = 4
N_TENSOR = 4


def make_pairs(key):
    key_draw = jnp.clip(jax.random.normal(jax.random.fold_in(key, 101), (TOKENS, KVH, HD), jnp.float32), -5.0, 5.0)
    query_draw = jax.random.normal(jax.random.fold_in(key, 202), (TOKENS, H, HD), jnp.float32)
    return (query_draw.reshape(TOKENS, H * HD), key_draw.reshape(TOKENS, KVH * HD))


def draw_query_rows(key, part):
    return make_pairs(key)[0].astype(jnp.bfloat16)


def draw_key_rows(key, part):
    return make_pairs(key)[1].astype(jnp.bfloat16)


def raised(result, own_key, source, target, shards_of, factor):
    def block_of(position):
        return (jnp.arange(result.shape[position]) // (result.shape[position] // shards_of)).reshape((-1,) + (1,) * (result.ndim - 1 - position))

    near = jax.random.permutation(own_key, shards_of)[block_of(target)]
    second = (block_of(target) + shards_of // 2) % shards_of
    return jnp.where((block_of(source) == near) | (block_of(source) == second), factor * result, result)


def shard_levels(rng, shape, split, least, largest):
    def one(axis_at, parts):
        heights = jax.random.uniform(jax.random.fold_in(jax.random.fold_in(rng, 6), axis_at), (parts,), jnp.float32, least / len(split), largest / len(split))
        return jnp.repeat(jnp.exp(heights), shape[axis_at] // parts).reshape((-1,) + (1,) * (len(shape) - axis_at - 1))

    gain = one(*split[0])
    for cut in split[1:]:
        gain = gain * one(*cut)
    return gain


def profile(amount, total, reach, lean):
    portions = [(1 << 20) // math.isqrt(standing ** lean) + 1 for standing in range(2, amount + 1)]
    spare, holding = total - reach - (amount - 1), [1] * (amount - 1)
    while spare > 0:
        candidates = [i for i in range(amount - 1) if holding[i] < reach]
        mass, left = sum([portions[i] for i in candidates]), spare
        for i in candidates:
            extra = min(reach - holding[i], max(1, left * portions[i] // mass), spare)
            holding[i] = holding[i] + extra
            spare = spare - extra
    return np.array([reach] + holding)


def ragged(own_key, number_of, total, limit, lean):
    if number_of == 2:
        one = jax.random.randint(own_key, (), max(1, total - limit), min(limit, total - 1) + 1)
        return jnp.stack([one, total - one])
    lengths = jnp.asarray(profile(number_of, total, limit, lean), jnp.int32)
    twos = (number_of - 1) // 2
    source_of, receiver = lengths[1:1 + 2 * twos:2], lengths[2:2 + 2 * twos:2]
    slack = jnp.minimum(source_of - 1, limit - receiver)
    shifted = jax.random.randint(jax.random.fold_in(own_key, 1), (twos,), 0, 1 << 20) % (slack + 1)
    lengths = lengths.at[1:1 + 2 * twos:2].set(source_of - shifted).at[2:2 + 2 * twos:2].set(receiver + shifted)
    return lengths[jax.random.permutation(jax.random.fold_in(own_key, 2), number_of)]


def normal_values(rng, shape, deviation, limit, cuts=(), kind=jnp.bfloat16):
    values = jax.random.normal(rng, shape, jnp.float32) * deviation
    if len(cuts) > 0:
        values = shard_levels(rng, shape, cuts, -0.22, 0.18) * values
    return jnp.clip(values, min=-limit, max=limit).astype(kind)


def bell_draw_with(stream_key, extent, width, most, cuts, heavy, kind=jnp.bfloat16):
    values = width * jax.random.normal(stream_key, extent, jnp.float32)
    if cuts:
        values = values * shard_levels(stream_key, extent, cuts, -0.22, 0.18)
    return jnp.clip(raised(values, jax.random.fold_in(stream_key, 3), *heavy), -most, most).astype(kind)


def setup_inputs(seed: int = 0) -> dict:
    key_of = jax.random.split(jax.random.key(seed), 6)
    return {
        "query_rows": draw_query_rows(jax.random.fold_in(key_of[5], 71), 0),
        "key_rows": draw_key_rows(jax.random.fold_in(key_of[5], 71), 0),
        "value_rows": normal_values(key_of[2], (TOKENS, KVH * HD), 1.0, 6.0, ((0, 8),)),
        "doc_ids": jnp.searchsorted(jnp.cumsum(ragged(key_of[3], DOCS, TOKENS, DOC_MOST, 2)), jnp.arange(TOKENS), side="right").astype(jnp.int32),
        "out_weight": bell_draw_with(key_of[4], (H * HD, D), (H * HD) ** -0.5, 0.09375, ((0, 4),), (0, 1, 4, 2.0)),
    }


def reference(query_rows, key_rows, value_rows, doc_ids, out_weight):
    group_size = H // KVH
    key_span = DOC_MOST + TOK_DEV
    padded_keys = jnp.pad(key_rows, ((DOC_MOST, 0), (0, 0)))
    padded_values = jnp.pad(value_rows, ((DOC_MOST, 0), (0, 0)))
    padded_docs = jnp.pad(doc_ids, (DOC_MOST, 0), constant_values=-1)

    def one_block(block_index):
        first_row = (block_index * TOK_DEV).astype(jnp.int32)
        block_queries = lax.dynamic_slice_in_dim(query_rows, first_row, TOK_DEV, 0)
        block_queries = block_queries.astype(jnp.float32).reshape(TOK_DEV, KVH, group_size, HD)
        window_keys = lax.dynamic_slice_in_dim(padded_keys, first_row, key_span, 0)
        window_keys = window_keys.astype(jnp.float32).reshape(key_span, KVH, HD)
        window_values = lax.dynamic_slice_in_dim(padded_values, first_row, key_span, 0)
        window_values = window_values.astype(jnp.float32).reshape(key_span, KVH, HD)
        window_docs = lax.dynamic_slice_in_dim(padded_docs, first_row, key_span, 0)
        query_docs = lax.dynamic_slice_in_dim(doc_ids, first_row, TOK_DEV, 0)
        query_pos = first_row + jnp.arange(TOK_DEV, dtype=jnp.int32)
        key_pos = first_row - DOC_MOST + jnp.arange(key_span, dtype=jnp.int32)
        allowed = (key_pos[None, :] <= query_pos[:, None]) & (window_docs[None, :] == query_docs[:, None])
        scores = jnp.einsum("tkgd,skd->kgts", block_queries, window_keys) * (HD ** -0.5)
        scores = jnp.where(allowed, scores, -jnp.inf)
        highest = jnp.max(scores, axis=-1, keepdims=True)
        weights = jnp.where(allowed, jnp.exp(scores - highest), 0.0)
        totals = jnp.sum(weights, axis=-1)
        rounded = lax.optimization_barrier(weights.astype(jnp.bfloat16)).astype(jnp.float32)
        numer = jnp.einsum("kgts,skd->kgtd", rounded, window_values)
        attended = numer / totals[..., None]
        return attended.transpose(2, 0, 1, 3).reshape(TOK_DEV, H * HD).astype(jnp.bfloat16)

    blocks = lax.map(one_block, jnp.arange(TOKENS // TOK_DEV, dtype=jnp.int32))
    attended = blocks.reshape(TOKENS, H * HD)
    local_width = (H // N_TENSOR) * HD

    def add_group(index, running):
        first_col = (index * local_width).astype(jnp.int32)
        columns = lax.dynamic_slice_in_dim(attended, first_col, local_width, 1)
        weight_rows = lax.dynamic_slice_in_dim(out_weight, first_col, local_width, 0)
        partial_value = jnp.dot(columns, weight_rows, preferred_element_type=jnp.float32)
        rounded = lax.optimization_barrier(partial_value.astype(jnp.bfloat16)).astype(jnp.float32)
        return running + rounded

    mixed = lax.fori_loop(0, N_TENSOR, add_group, jnp.zeros((TOKENS, D), jnp.float32))
    return mixed.astype(jnp.bfloat16)
```

```python
import functools
import math

import jax
import jax.numpy as jnp
from jax import lax
from jax.experimental import pallas as pl
from jax.experimental.pallas import tpu as pltpu
from jax.sharding import PartitionSpec as P

H = 64
KVH = 8
HD = 128
DOC_MOST = 1024
REACH = 4
NEG_BIG = -1e30
MESH = pl.DeviceIdType.MESH
CHUNK = 512


def kernel(
    n_tensor, n_context, kv_count, per_kv, steps, chunks,
    query_hbm, key_hbm, value_hbm, doc_ref, weight_hbm, out_ref,
    query, kv, docs, bias, run_top, run_sum, att, weight, own, pair_out, pair_in, chip_out, chip_in,
    load_sem, kv_load_sem, weight_sem, kv_send, kv_recv, doc_send, doc_recv,
    pair_send, pair_recv, chip_send, chip_recv,
):
    tensor = lax.axis_index("tensor")
    context = lax.axis_index("context")
    chip, core = tensor // 2, tensor % 2
    partner = chip * 2 + (1 - core)
    n_chip = n_tensor // 2
    tok = query.shape[0]
    half = tok // 2
    cols = chunks * own.shape[-1]
    width = own.shape[-1]
    even = context % 2 == 0
    odd = context % 2 == 1
    ahead = context + 2 < n_context
    first_kv = tensor * (kv_count * per_kv) // (H // KVH) if per_kv * kv_count < H // KVH else tensor * kv_count

    def place(d):
        return (REACH - d) * tok

    kv_loads = []
    for g in range(kv_count):
        at = pl.ds(pl.multiple_of((first_kv + g) * HD, HD), HD)
        mine = kv.at[g, pl.ds(place(0), tok)]
        pair = (
            pltpu.make_async_copy(key_hbm.at[:, at], mine.at[:, pl.ds(0, HD)], kv_load_sem.at[g, 0]),
            pltpu.make_async_copy(value_hbm.at[:, at], mine.at[:, pl.ds(HD, HD)], kv_load_sem.at[g, 1]),
        )
        for c in pair:
            c.start()
        kv_loads.append(pair)
    query_load = pltpu.make_async_copy(query_hbm, query, load_sem)
    query_load.start()

    barrier = pltpu.get_barrier_semaphore()
    heard = jnp.int32(n_chip)
    for d in range(1, REACH + 1):
        for away in (d, -d):
            there = context + away
            ok = (there >= 0) & (there < n_context)
            heard = heard + jnp.where(ok, 1, 0).astype(jnp.int32)

            @pl.when(ok)
            def _():
                pl.semaphore_signal(barrier, inc=1, device_id={"tensor": tensor, "context": there}, device_id_type=MESH)

    pl.semaphore_signal(barrier, inc=1, device_id={"tensor": partner, "context": context}, device_id_type=MESH)
    for d in range(1, n_chip):
        to = lax.rem(chip + d, n_chip) * 2 + core
        pl.semaphore_signal(barrier, inc=1, device_id={"tensor": to, "context": context}, device_id_type=MESH)
    pl.semaphore_wait(barrier, heard)

    parts = 2 * kv_count
    by_even = range(parts // 2)
    by_odd = range(parts // 2, parts)
    later_first = sorted(range(parts), key=lambda q: 1 - q % 2)

    def kv_copy(q, from_d, to_d, kind, there):
        g, h = q // 2, q % 2
        return pltpu.make_async_remote_copy(
            src_ref=kv.at[g, pl.ds(place(from_d) + h * half, half)],
            dst_ref=kv.at[g, pl.ds(place(to_d) + h * half, half)],
            send_sem=kv_send.at[kind, q],
            recv_sem=kv_recv.at[to_d - 1, q],
            device_id={"tensor": tensor, "context": there},
            device_id_type=MESH,
        )

    def hops(q):
        near = context >= 2
        far = context >= 4
        here = [
            (ahead, lambda: kv_copy(q, 0, 2, 0, context + 2)),
            (even, lambda: kv_copy(q, 0, 1, 1, context + 1)),
            (even & near, lambda: kv_copy(q, 2, 3, 2, context + 1)),
            (odd & near, lambda: kv_copy(q, 2, 1, 2, context - 1)),
            (near & ahead, lambda: kv_copy(q, 2, 4, 3, context + 2)),
        ]
        if q in by_even:
            here.append((even & near & ahead, lambda: kv_copy(q, 1, 3, 4, context + 2)))
        else:
            here.append((odd & far, lambda: kv_copy(q, 4, 3, 4, context - 1)))
        return here

    def launch(q, hop, *also):
        ok, c = hops(q)[hop]
        for more in also:
            ok = ok & more

        @pl.when(ok)
        def _():
            c().start()

    def arrive(d, q, *also):
        ok = context >= d
        for more in also:
            ok = ok & more

        @pl.when(ok)
        def _():
            kv_copy(q, 0, d, 0, context).wait_recv()

    def doc_copy(d):
        return pltpu.make_async_remote_copy(
            src_ref=doc_ref,
            dst_ref=docs.at[REACH - d],
            send_sem=doc_send.at[d - 1],
            recv_sem=doc_recv.at[d - 1],
            device_id={"tensor": tensor, "context": context + d},
            device_id_type=MESH,
        )

    for d in range(1, REACH + 1):
        @pl.when(context + d < n_context)
        def _():
            doc_copy(d).start()

    for g in range(kv_count):
        for c in kv_loads[g]:
            c.wait()
        for q in (2 * g, 2 * g + 1):
            launch(q, 0)
            launch(q, 1)

    def weight_copy(i, side):
        to = lax.rem(chip + 1 + i // chunks, n_chip) * 2 + (core if side == 0 else 1 - core)
        at = to * cols + lax.rem(i, chunks) * width
        return pltpu.make_async_copy(
            weight_hbm.at[:, pl.ds(pl.multiple_of(at, 128), width)], weight.at[i, side], weight_sem.at[i, side]
        )

    @pl.loop(0, steps)
    def _(i):
        weight_copy(i, 1).start()
        weight_copy(i, 0).start()

    scale = HD ** -0.5 * math.log2(math.e)

    def columns(head):
        return pl.ds(pl.multiple_of(head * HD, HD), HD)

    def attend(g, h, r, start, size, first, last):
        rows = pl.ds(r * half, half)
        keys = pl.ds(start, size)
        heads = (g * per_kv + 2 * h, g * per_kv + 2 * h + 1)
        at = g * (per_kv // 2) + h
        q = jnp.concatenate([query[rows, columns(head)] for head in heads], axis=0)
        scores = lax.dot_general(
            q, kv[g, keys, :HD], (((1,), (1,)), ((), ())), preferred_element_type=jnp.float32
        ) + jnp.concatenate([bias[rows, keys]] * 2, axis=0)
        top = jnp.max(scores, axis=-1, keepdims=True)
        if not first:
            before = run_top[at, r][:, :1]
            top = jnp.maximum(top, before)
        values = kv[g, keys, HD:]
        both = jnp.concatenate([values, jnp.ones_like(values)], axis=1)
        p = jnp.exp2((scores - top) * scale).astype(jnp.bfloat16)
        sums = jnp.dot(p, both, preferred_element_type=jnp.float32)
        if not first:
            sums = sums + jnp.exp2((before - top) * scale) * run_sum[at, r]
        if last:
            done = (sums[:, :HD] / sums[:, HD:]).astype(jnp.bfloat16)
            att[rows, columns(heads[0])] = done[:half]
            att[rows, columns(heads[1])] = done[half:]
        else:
            run_top[at, r] = jnp.broadcast_to(top, (tok, HD))
            run_sum[at, r] = sums

    def attend_all(g, r, start, size, first, last):
        @pl.loop(0, per_kv // 2, unroll=min(2, per_kv // 2))
        def _(h):
            attend(g, h, r, start, size, first, last)

    doc_row = doc_ref[...].astype(jnp.float32)
    doc_col = jnp.broadcast_to(doc_row, (tok, tok)).T
    causal = lax.broadcasted_iota(jnp.int32, (tok, tok), 1) <= lax.broadcasted_iota(jnp.int32, (tok, tok), 0)
    bias[:, pl.ds(place(0), tok)] = jnp.where(causal & (doc_col == doc_row), 0.0, NEG_BIG)
    query_load.wait()
    for g in range(kv_count):
        attend_all(g, 1, place(0), tok, True, False)
        attend_all(g, 0, place(0), half, True, False)

    for d in range(1, REACH + 1):
        @pl.when(context < d)
        def _():
            docs[REACH - d] = jnp.full(docs.shape[1:], -1, jnp.int32)
            for g in range(kv_count):
                kv[g, pl.ds(place(d), tok)] = jnp.zeros((tok, 2 * HD), kv.dtype)

        @pl.when(context >= d)
        def _():
            doc_copy(d).wait_recv()

    for d in range(1, REACH + 1):
        row = docs[REACH - d].astype(jnp.float32)
        bias[:, pl.ds(place(d), tok)] = jnp.where(doc_col == row, 0.0, NEG_BIG)

    lag = 2
    for q in range(max(parts, lag + len(by_even))):
        if q < parts:
            arrive(2, q)
            launch(q, 2)
            launch(q, 3)
            if q in by_odd:
                launch(q, 4, odd)
        if q - lag in by_even:
            arrive(1, q - lag, even)
            launch(q - lag, 5)
    for q in later_first:
        launch(q, 4, even) if q in by_odd else launch(q, 4)

    def middle(g, r):
        attend_all(g, r, place(3) + tok, 2 * tok, False, False)

    def distant(g, r):
        skip = half * r
        attend_all(g, r, skip, 2 * tok - skip, False, True)

    def middle_arrive(g):
        for q in (2 * g, 2 * g + 1):
            arrive(1, q, odd) if q in by_even else arrive(1, q)

    def relay_far(q):
        arrive(4, q, odd)
        launch(q, 5)

    waiting = [(g, r) for g in range(kv_count) for r in (1, 0)]
    late = waiting.pop() if kv_count > 1 else None
    relays = list(by_odd)
    for g, r in waiting:
        if r == 1:
            middle_arrive(g)
        middle(g, r)
        if relays:
            relay_far(relays.pop(0))
    for q in relays:
        relay_far(q)

    def distant_arrive(g, r):
        if r == 1:
            arrive(3, 2 * g)
            arrive(3, 2 * g + 1)
        q = 2 * g + r
        arrive(4, q, even) if q in by_odd else arrive(4, q)

    def pair_copy(i, rows, k):
        return pltpu.make_async_remote_copy(
            src_ref=pair_out.at[i, rows], dst_ref=pair_in.at[i, rows],
            send_sem=pair_send.at[i, k], recv_sem=pair_recv.at[i, k],
            device_id={"tensor": partner, "context": context}, device_id_type=MESH,
        )

    def chip_copy(i, r):
        to = lax.rem(chip + 1 + i // chunks, n_chip) * 2 + core
        rows = pl.ds(r * half, half)
        return pltpu.make_async_remote_copy(
            src_ref=chip_out.at[i, rows], dst_ref=chip_in.at[i, rows],
            send_sem=chip_send.at[i, r], recv_sem=chip_recv.at[i, r],
            device_id={"tensor": to, "context": context}, device_id_type=MESH,
        )

    away = steps - chunks

    def project(i, rows, k, first):
        if first:
            weight_copy(i, 1).wait()
        pair_out[i, rows] = jnp.dot(att[rows, :], weight[i, 1], preferred_element_type=jnp.float32).astype(jnp.bfloat16)
        pair_copy(i, rows, k).start()
        if first:
            weight_copy(i, 0).wait()
        own[i, rows] = jnp.dot(att[rows, :], weight[i, 0], preferred_element_type=jnp.float32).astype(jnp.bfloat16)

    def forward(i, r):
        rows = pl.ds(r * half, half)
        pair_copy(i, rows, r).wait_recv()
        both = own[i, rows].astype(jnp.float32) + pair_in[i, rows].astype(jnp.float32)
        chip_out[i, rows] = both.astype(jnp.bfloat16)
        chip_copy(i, r).start()

    for r in (1, 0):
        rows = pl.ds(r * half, half)
        if r == 0 and late is not None:
            middle(*late)
        for g in range(kv_count):
            distant_arrive(g, r)
            distant(g, r)

        project(0, rows, r, r == 1)

        @pl.loop(1, away)
        def _(i):
            project(i, rows, r, r == 1)
            forward(i - 1, r)

        forward(away - 1, r)

    every = pl.ds(0, tok)
    @pl.loop(away, steps)
    def _(i):
        project(i, every, 0, True)

    for j in range(chunks):
        pair_copy(away + j, every, 0).wait_recv()
    for r in (1, 0):
        for j in range(chunks):
            rows = pl.ds(r * half, half)
            both = own[away + j, rows].astype(jnp.float32) + pair_in[away + j, rows].astype(jnp.float32)
            for d in range(n_chip - 1):
                chip_copy(d * chunks + j, r).wait_recv()
            for d in range(n_chip - 1):
                both = both + chip_in[d * chunks + j, rows].astype(jnp.float32)
            out_ref[rows, pl.ds(j * width, width)] = both.astype(out_ref.dtype)

    for d in range(1, REACH + 1):
        @pl.when(context + d < n_context)
        def _():
            doc_copy(d).wait_send()
    for q in range(parts):
        for ok, c in hops(q):
            @pl.when(ok)
            def _():
                c().wait_send()

    @pl.loop(0, away)
    def _(i):
        for r in range(2):
            pair_copy(i, pl.ds(r * half, half), r).wait_send()
            chip_copy(i, r).wait_send()

    @pl.loop(away, steps)
    def _(i):
        pair_copy(i, every, 0).wait_send()


def body(n_tensor, n_context, query_rows, key_rows, value_rows, doc_ids, out_weight):
    tok, local = query_rows.shape
    local_heads = local // HD
    group_size = H // KVH
    kv_count = max(1, local_heads // group_size)
    per_kv = local_heads // kv_count
    model = out_weight.shape[1]
    cols = model // n_tensor
    width = min(CHUNK, cols)
    chunks = cols // width
    n_chip = n_tensor // 2
    steps = n_chip * chunks
    assert n_tensor % 2 == 0 and n_context % 2 == 0 and cols % width == 0 and n_tensor > 2 and per_kv % 2 == 0 and tok % 2 == 0
    assert REACH * tok >= DOC_MOST - 1
    bf = jnp.bfloat16
    dma = pltpu.SemaphoreType.DMA
    anywhere = pl.BlockSpec(memory_space=pl.ANY)
    inside = pl.BlockSpec(memory_space=pltpu.VMEM)
    away = steps - chunks
    return pl.pallas_call(
        functools.partial(kernel, n_tensor, n_context, kv_count, per_kv, steps, chunks),
        out_shape=pltpu.VMEM((tok, cols), bf),
        in_specs=[anywhere, anywhere, anywhere, inside, anywhere],
        out_specs=inside,
        scratch_shapes=[
            pltpu.VMEM((tok, local), bf),
            pltpu.VMEM((kv_count, (REACH + 1) * tok, 2 * HD), bf),
            pltpu.VMEM((REACH, 1, tok), jnp.int32),
            pltpu.VMEM((tok, (REACH + 1) * tok), jnp.float32),
            pltpu.VMEM((local_heads // 2, 2, tok, HD), jnp.float32),
            pltpu.VMEM((local_heads // 2, 2, tok, 2 * HD), jnp.float32),
            pltpu.VMEM((tok, local), bf),
            pltpu.VMEM((steps, 2, local, width), bf),
            pltpu.VMEM((steps, tok, width), bf),
            pltpu.VMEM((steps, tok, width), bf),
            pltpu.VMEM((steps, tok, width), bf),
            pltpu.VMEM((max(away, 1), tok, width), bf),
            pltpu.VMEM((max(away, 1), tok, width), bf),
            dma,
            dma((kv_count, 2)),
            dma((steps, 2)),
            dma((5, 2 * kv_count)),
            dma((REACH, 2 * kv_count)),
            dma((REACH,)),
            dma((REACH,)),
            dma((steps, 2)),
            dma((steps, 2)),
            dma((max(away, 1), 2)),
            dma((max(away, 1), 2)),
        ],
        compiler_params=pltpu.CompilerParams(
            collective_id=0, has_side_effects=True, vmem_limit_bytes=57 * 1024 * 1024
        ),
    )(query_rows, key_rows, value_rows, doc_ids.reshape(1, tok), out_weight)


def solution(mesh):
    placed = (
        P("context", "tensor"),
        P("context", None),
        P("context", None),
        P("context"),
        P("tensor", None),
    )
    return jax.shard_map(
        functools.partial(body, mesh.shape["tensor"], mesh.shape["context"]),
        mesh=mesh, in_specs=placed, out_specs=P("context", "tensor"), check_vma=False,
    )
```

```python
import functools
import math

import jax
import jax.numpy as jnp
from jax import lax
from jax.experimental import pallas as pl
from jax.experimental.pallas import tpu as pltpu
from jax.sharding import PartitionSpec as P

H = 64
KVH = 8
HD = 128
DOC_MOST = 1024
REACH = 4
CUTS = 4
NEG_BIG = -1e30
MESH = pl.DeviceIdType.MESH
CHUNK = 512


def kernel(
    n_tensor, n_context, kv_count, per_kv, steps, chunks,
    query_hbm, key_hbm, value_hbm, doc_ref, weight_hbm, out_ref,
    query, kv, docs, bias, run_top, run_sum, att, weight, own, pair_out, pair_in, chip_out, chip_in,
    load_sem, kv_load_sem, weight_sem, kv_send, kv_recv, doc_send, doc_recv,
    pair_send, pair_recv, chip_send, chip_recv,
):
    tensor = lax.axis_index("tensor")
    context = lax.axis_index("context")
    chip, core = tensor // 2, tensor % 2
    partner = chip * 2 + (1 - core)
    n_chip = n_tensor // 2
    tok = query.shape[0]
    half = tok // 2
    cols = chunks * own.shape[-1]
    width = own.shape[-1]
    even = context % 2 == 0
    odd = context % 2 == 1
    ahead = context + 2 < n_context
    first_kv = tensor * (kv_count * per_kv) // (H // KVH) if per_kv * kv_count < H // KVH else tensor * kv_count

    def place(d):
        return (REACH - d) * tok

    kv_loads = []
    for g in range(kv_count):
        at = pl.ds(pl.multiple_of((first_kv + g) * HD, HD), HD)
        mine = kv.at[g, pl.ds(place(0), tok)]
        pair = (
            pltpu.make_async_copy(key_hbm.at[:, at], mine.at[:, pl.ds(0, HD)], kv_load_sem.at[g, 0]),
            pltpu.make_async_copy(value_hbm.at[:, at], mine.at[:, pl.ds(HD, HD)], kv_load_sem.at[g, 1]),
        )
        for c in pair:
            c.start()
        kv_loads.append(pair)
    query_load = pltpu.make_async_copy(query_hbm, query, load_sem)
    query_load.start()

    barrier = pltpu.get_barrier_semaphore()
    beside = context + 1 - 2 * (context % 2)
    heard = jnp.int32(n_chip + 1)
    pl.semaphore_signal(barrier, inc=1, device_id={"tensor": tensor, "context": beside}, device_id_type=MESH)
    for there in (context + 2, context - 2):
        ok = (there >= 0) & (there < n_context)
        heard = heard + jnp.where(ok, 1, 0).astype(jnp.int32)

        @pl.when(ok)
        def _():
            pl.semaphore_signal(barrier, inc=1, device_id={"tensor": tensor, "context": there}, device_id_type=MESH)

    pl.semaphore_signal(barrier, inc=1, device_id={"tensor": partner, "context": context}, device_id_type=MESH)
    for d in range(1, n_chip):
        to = lax.rem(chip + d, n_chip) * 2 + core
        pl.semaphore_signal(barrier, inc=1, device_id={"tensor": to, "context": context}, device_id_type=MESH)
    pl.semaphore_wait(barrier, heard)

    parts = CUTS * kv_count
    piece = tok // CUTS
    by_odd = range(parts // 4, parts - parts // 4)
    by_even = [q for q in range(parts) if q not in by_odd]
    later = [q for q in range(parts) if q % CUTS >= CUTS // 2]
    near = context >= 2
    far = context >= 4

    def kv_copy(q, from_d, to_d, kind, there):
        g, t = q // CUTS, q % CUTS
        return pltpu.make_async_remote_copy(
            src_ref=kv.at[g, pl.ds(place(from_d) + t * piece, piece)],
            dst_ref=kv.at[g, pl.ds(place(to_d) + t * piece, piece)],
            send_sem=kv_send.at[kind, q],
            recv_sem=kv_recv.at[to_d - 1, q],
            device_id={"tensor": tensor, "context": there},
            device_id_type=MESH,
        )

    def doc_copy(from_d, to_d, kind, there):
        return pltpu.make_async_remote_copy(
            src_ref=docs.at[REACH - from_d] if from_d else doc_ref,
            dst_ref=docs.at[REACH - to_d],
            send_sem=doc_send.at[kind],
            recv_sem=doc_recv.at[to_d - 1],
            device_id={"tensor": tensor, "context": there},
            device_id_type=MESH,
        )

    def routes(q):
        here = [
            (ahead, 0, 2, 0, context + 2),
            (even, 0, 1, 1, context + 1),
            (even & near, 2, 3, 2, context + 1),
            (odd & near, 2, 1, 2, context - 1),
            (near & ahead, 2, 4, 3, context + 2),
        ]
        if q is None or q in by_even:
            here.append((even & near & ahead, 1, 3, 4, context + 2))
        else:
            here.append((odd & far, 4, 3, 4, context - 1))
        return here

    def hops(q):
        if q is None:
            return [(ok, functools.partial(doc_copy, *way)) for ok, *way in routes(q)]
        return [(ok, functools.partial(kv_copy, q, *way)) for ok, *way in routes(q)]

    def launch_all(q, *which):
        for hop in which:
            launch(q, hop)

    def launch(q, hop, *also):
        ok, c = hops(q)[hop]
        for more in also:
            ok = ok & more

        @pl.when(ok)
        def _():
            c().start()

    def arrive(d, q, *also):
        ok = context >= d
        for more in also:
            ok = ok & more

        @pl.when(ok)
        def _():
            kv_copy(q, 0, d, 0, context).wait_recv()

    def doc_arrive(d, *also):
        ok = context >= d
        for more in also:
            ok = ok & more

        @pl.when(ok)
        def _():
            doc_copy(0, d, 0, context).wait_recv()

    launch_all(None, 0, 1)
    for g in range(kv_count):
        for c in kv_loads[g]:
            c.wait()
        for q in range(CUTS * g, CUTS * (g + 1)):
            launch_all(q, 0, 1)

    def weight_copy(i, side):
        to = lax.rem(chip + 1 + i // chunks, n_chip) * 2 + (core if side == 0 else 1 - core)
        at = to * cols + lax.rem(i, chunks) * width
        return pltpu.make_async_copy(
            weight_hbm.at[:, pl.ds(pl.multiple_of(at, 128), width)], weight.at[i, side], weight_sem.at[i, side]
        )

    @pl.loop(0, steps)
    def _(i):
        weight_copy(i, 1).start()
        weight_copy(i, 0).start()

    scale = HD ** -0.5 * math.log2(math.e)

    def columns(head):
        return pl.ds(pl.multiple_of(head * HD, HD), HD)

    def attend(g, h, r, start, size, first, last):
        rows = pl.ds(r * half, half)
        keys = pl.ds(start, size)
        heads = (g * per_kv + 2 * h, g * per_kv + 2 * h + 1)
        at = g * (per_kv // 2) + h
        q = jnp.concatenate([query[rows, columns(head)] for head in heads], axis=0)
        scores = lax.dot_general(
            q, kv[g, keys, :HD], (((1,), (1,)), ((), ())), preferred_element_type=jnp.float32
        ) + jnp.concatenate([bias[rows, keys]] * 2, axis=0)
        top = jnp.broadcast_to(jnp.max(scores, axis=-1, keepdims=True), (tok, HD))
        if not first:
            before = run_top[at, r]
            top = jnp.maximum(top, before)
        values = kv[g, keys, HD:]
        both = jnp.concatenate([values, jnp.ones_like(values)], axis=1)
        p = jnp.exp2((scores - jnp.concatenate([top] * (size // HD), axis=1)) * scale).astype(jnp.bfloat16)
        sums = jnp.dot(p, both, preferred_element_type=jnp.float32)
        if not first:
            fade = jnp.exp2((before - top) * scale)
            sums = sums + jnp.concatenate([fade, fade], axis=1) * run_sum[at, r]
        if last:
            done = (sums[:, :HD] / sums[:, HD:]).astype(jnp.bfloat16)
            att[rows, columns(heads[0])] = done[:half]
            att[rows, columns(heads[1])] = done[half:]
        else:
            run_top[at, r] = top
            run_sum[at, r] = sums

    def attend_all(g, r, start, size, first, last):
        @pl.loop(0, per_kv // 2, unroll=min(4, per_kv // 2))
        def _(h):
            attend(g, h, r, start, size, first, last)

    doc_row = doc_ref[...].astype(jnp.float32)
    doc_col = jnp.broadcast_to(doc_row, (tok, tok)).T
    causal = lax.broadcasted_iota(jnp.int32, (tok, tok), 1) <= lax.broadcasted_iota(jnp.int32, (tok, tok), 0)
    bias[:, pl.ds(place(0), tok)] = jnp.where(causal & (doc_col == doc_row), 0.0, NEG_BIG)
    query_load.wait()
    for g in range(kv_count):
        attend_all(g, 1, place(0), tok, True, False)
        attend_all(g, 0, place(0), tok, True, False)

    def mask(d, where=True):
        @pl.when(where & (context < d))
        def _():
            docs[REACH - d] = jnp.full(docs.shape[1:], -1, jnp.int32)
            for g in range(kv_count):
                kv[g, pl.ds(place(d), tok)] = jnp.zeros((tok, 2 * HD), kv.dtype)

        @pl.when(where & (context < n_context))
        def _():
            row = docs[REACH - d].astype(jnp.float32)
            bias[:, pl.ds(place(d), tok)] = jnp.where(doc_col == row, 0.0, NEG_BIG)

    doc_arrive(2)
    launch_all(None, 2, 3, 4)
    mask(2)

    lag = CUTS + 1
    sent = []

    def relay_even(q):
        arrive(1, q, even)
        launch(q, 5)

    def middle(g, r):
        attend_all(g, r, place(2), 2 * tok, False, False)

    def distant(g, r):
        skip = half * r
        attend_all(g, r, skip, 2 * tok - skip, False, True)

    def middle_arrive(g, where):
        for q in range(CUTS * g, CUTS * (g + 1)):
            if q in by_odd:
                arrive(1, q, where)
                continue
            if where is not even:
                arrive(1, q, odd)
            if where is not odd and q in turns:
                turns.remove(q)
                relay_even(q)

    def odd_middle(r):
        @pl.when(odd)
        def _():
            if r == 1:
                middle_arrive(0, odd)
            middle(0, r)

    odd_turns = [(CUTS - 1, 1), (min(parts - 1, CUTS + 1), 0)]
    turns = list(by_even)
    queue = list(later)
    for q in range(parts):
        arrive(2, q)
        launch_all(q, 2, 3)
        if q in by_odd:
            launch(q, 4, odd)
        if q >= lag and turns and turns[0] <= q - lag:
            relay_even(turns.pop(0))
        elif queue and queue[0] <= q:
            sent.append(queue.pop(0))
            launch(sent[-1], 4, even)
        if q == CUTS - 1:
            doc_arrive(1, odd)
            mask(1, odd)
        for turn, r in odd_turns:
            if q == turn:
                odd_middle(r)
        if q == (3 * parts) // 4:
            doc_arrive(1, even)
            launch(None, 5)
    for q in sorted(by_even, key=lambda q: q not in later):
        launch(q, 4, odd)
    for q in queue:
        launch(q, 4, even)
    rest = [q for q in range(parts) if q not in later]
    launch(rest[0], 4, even)

    def relay_far(q):
        arrive(4, q, odd)
        launch(q, 5)

    relays = list(by_odd)
    for q in relays[: len(relays) // 2]:
        relay_far(q)
    mask(1, even)
    doc_arrive(4)
    mask(4)

    @pl.when(even)
    def _():
        middle_arrive(0, even)
        for r in (1, 0):
            middle(0, r)

    late = (kv_count - 1, 0) if kv_count > 1 else None
    for g in range(1, kv_count):
        middle_arrive(g, True)
        middle(g, 1)
        if g < kv_count - 1:
            middle(g, 0)
    for q in rest[1:]:
        launch(q, 4, even)
    for q in relays[len(relays) // 2 :]:
        relay_far(q)
    doc_arrive(3)
    mask(3)

    def distant_arrive(g, r):
        for q in range(CUTS * g, CUTS * (g + 1)):
            if r == 1:
                arrive(3, q)
            if (q in later) == (r == 1):
                arrive(4, q, even) if q in by_odd else arrive(4, q)

    def pair_copy(i, rows, k):
        return pltpu.make_async_remote_copy(
            src_ref=pair_out.at[i, rows], dst_ref=pair_in.at[i, rows],
            send_sem=pair_send.at[i, k], recv_sem=pair_recv.at[i, k],
            device_id={"tensor": partner, "context": context}, device_id_type=MESH,
        )

    def chip_copy(i, r):
        to = lax.rem(chip + 1 + i // chunks, n_chip) * 2 + core
        rows = pl.ds(r * half, half)
        return pltpu.make_async_remote_copy(
            src_ref=chip_out.at[i, rows], dst_ref=chip_in.at[i, rows],
            send_sem=chip_send.at[i, r], recv_sem=chip_recv.at[i, r],
            device_id={"tensor": to, "context": context}, device_id_type=MESH,
        )

    away = steps - chunks

    def give(i, rows, k, first):
        if first:
            weight_copy(i, 1).wait()
        pair_out[i, rows] = jnp.dot(att[rows, :], weight[i, 1], preferred_element_type=jnp.float32).astype(jnp.bfloat16)
        pair_copy(i, rows, k).start()

    def keep(i, rows, first):
        if first:
            weight_copy(i, 0).wait()
        own[i, rows] = jnp.dot(att[rows, :], weight[i, 0], preferred_element_type=jnp.float32).astype(jnp.bfloat16)

    def forward(i, r):
        rows = pl.ds(r * half, half)
        pair_copy(i, rows, r).wait_recv()
        both = own[i, rows].astype(jnp.float32) + pair_in[i, rows].astype(jnp.float32)
        chip_out[i, rows] = both.astype(jnp.bfloat16)
        chip_copy(i, r).start()

    for r in (1, 0):
        rows = pl.ds(r * half, half)
        if r == 0 and late is not None:
            middle(*late)
        for g in range(kv_count):
            distant_arrive(g, r)
            distant(g, r)

        give(0, rows, r, r == 1)
        keep(0, rows, r == 1)

        @pl.loop(1, away)
        def _(i):
            give(i, rows, r, r == 1)
            forward(i - 1, r)
            keep(i, rows, r == 1)

        forward(away - 1, r)

    every = pl.ds(0, tok)
    @pl.loop(away, steps)
    def _(i):
        give(i, every, 0, True)
        keep(i, every, True)

    for q in (None, *range(parts)):
        for ok, c in hops(q):
            @pl.when(ok)
            def _():
                c().wait_send()

    @pl.loop(0, away)
    def _(i):
        for r in range(2):
            pair_copy(i, pl.ds(r * half, half), r).wait_send()

    @pl.loop(away, steps)
    def _(i):
        pair_copy(i, every, 0).wait()

    for r in (1, 0):
        for j in range(chunks):
            rows = pl.ds(r * half, half)
            both = own[away + j, rows].astype(jnp.float32) + pair_in[away + j, rows].astype(jnp.float32)
            for d in range(n_chip - 1):
                chip_copy(d * chunks + j, r).wait_recv()
            for d in range(n_chip - 1):
                both = both + chip_in[d * chunks + j, rows].astype(jnp.float32)
            out_ref[rows, pl.ds(j * width, width)] = both.astype(out_ref.dtype)

    @pl.loop(0, away)
    def _(i):
        for r in range(2):
            chip_copy(i, r).wait_send()


def body(n_tensor, n_context, query_rows, key_rows, value_rows, doc_ids, out_weight):
    tok, local = query_rows.shape
    local_heads = local // HD
    group_size = H // KVH
    kv_count = max(1, local_heads // group_size)
    per_kv = local_heads // kv_count
    model = out_weight.shape[1]
    cols = model // n_tensor
    width = min(CHUNK, cols)
    chunks = cols // width
    n_chip = n_tensor // 2
    steps = n_chip * chunks
    assert n_tensor % 2 == 0 and n_context % 2 == 0 and cols % width == 0 and n_tensor > 2 and per_kv % 2 == 0 and tok % CUTS == 0
    assert REACH * tok >= DOC_MOST - 1
    bf = jnp.bfloat16
    dma = pltpu.SemaphoreType.DMA
    anywhere = pl.BlockSpec(memory_space=pl.ANY)
    inside = pl.BlockSpec(memory_space=pltpu.VMEM)
    away = steps - chunks
    return pl.pallas_call(
        functools.partial(kernel, n_tensor, n_context, kv_count, per_kv, steps, chunks),
        out_shape=pltpu.VMEM((tok, cols), bf),
        in_specs=[anywhere, anywhere, anywhere, inside, anywhere],
        out_specs=inside,
        scratch_shapes=[
            pltpu.VMEM((tok, local), bf),
            pltpu.VMEM((kv_count, (REACH + 1) * tok, 2 * HD), bf),
            pltpu.VMEM((REACH, 1, tok), jnp.int32),
            pltpu.VMEM((tok, (REACH + 1) * tok), jnp.float32),
            pltpu.VMEM((local_heads // 2, 2, tok, HD), jnp.float32),
            pltpu.VMEM((local_heads // 2, 2, tok, 2 * HD), jnp.float32),
            pltpu.VMEM((tok, local), bf),
            pltpu.VMEM((steps, 2, local, width), bf),
            pltpu.VMEM((steps, tok, width), bf),
            pltpu.VMEM((steps, tok, width), bf),
            pltpu.VMEM((steps, tok, width), bf),
            pltpu.VMEM((max(away, 1), tok, width), bf),
            pltpu.VMEM((max(away, 1), tok, width), bf),
            dma,
            dma((kv_count, 2)),
            dma((steps, 2)),
            dma((5, CUTS * kv_count)),
            dma((REACH, CUTS * kv_count)),
            dma((5,)),
            dma((REACH,)),
            dma((steps, 2)),
            dma((steps, 2)),
            dma((max(away, 1), 2)),
            dma((max(away, 1), 2)),
        ],
        compiler_params=pltpu.CompilerParams(
            collective_id=0, has_side_effects=True, vmem_limit_bytes=57 * 1024 * 1024
        ),
    )(query_rows, key_rows, value_rows, doc_ids.reshape(1, tok), out_weight)


def solution(mesh):
    placed = (
        P("context", "tensor"),
        P("context", None),
        P("context", None),
        P("context"),
        P("tensor", None),
    )
    return jax.shard_map(
        functools.partial(body, mesh.shape["tensor"], mesh.shape["context"]),
        mesh=mesh, in_specs=placed, out_specs=P("context", "tensor"), check_vma=False,
    )
```
